32 devices in a mesh: trial: 4 (over x, core), shard: 4 (over z), tp: 2 (over y).
Axes of the slice: x: 2, y: 2, z: 4, core: 2. Of those that a mesh axis runs over, the one named last changes fastest.
Arguments:
- weight_query: bfloat16 [10240, 4096], P(('trial', 'shard'), 'tp'), parts along dimension 0, may hold values from -0.125 to 0.125
- low_query: bfloat16 [10240, 64], P(('trial', 'shard')), parts along dimension 0, may hold values from -0.125 to 0.125
- high_query: bfloat16 [256, 4096], P('trial', 'tp'), parts along dimension 0, may hold values from -0.75 to 0.75
- weight_key: bfloat16 [10240, 1024], P(('trial', 'shard'), 'tp'), parts along dimension 0, may hold values from -0.125 to 0.125
- low_key: bfloat16 [10240, 64], P(('trial', 'shard')), parts along dimension 0, may hold values from -0.125 to 0.125
- high_key: bfloat16 [256, 1024], P('trial', 'tp'), parts along dimension 0, may hold values from -0.75 to 0.75
- weight_value: bfloat16 [10240, 1024], P(('trial', 'shard'), 'tp'), parts along dimension 0, may hold values from -0.125 to 0.125
- low_value: bfloat16 [10240, 64], P(('trial', 'shard')), parts along dimension 0, may hold values from -0.125 to 0.125
- high_value: bfloat16 [256, 1024], P('trial', 'tp'), parts along dimension 0, may hold values from -0.75 to 0.75
- norm_train: float32 [10240], P(('trial', 'shard', 'tp')), parts along dimension 0, may hold values from 0.25 to 1.75
- norm_step: float32 [10240], P(('trial', 'shard', 'tp')), parts along dimension 0, may hold values from -0.3 to 0.3
Outputs:
- serve_query: bfloat16 [16384, 2560], P(('trial', 'tp')), parts along dimension 0
- serve_key: bfloat16 [4096, 2560], P(('trial', 'tp')), parts along dimension 0
- serve_value: bfloat16 [4096, 2560], P(('trial', 'tp')), parts along dimension 0
- serve_norm: bfloat16 [10240], P('trial'), parts along dimension 0
The draws below stay inside these ranges and needn't reach their ends.
There are 4 independent parts, one for each index of `trial`. The reference program is written for one: setup_inputs(seed, part) draws one part's arguments, and reference() takes and returns one part's arrays. A program takes and returns all parts, laid end to end along the dimension named above; each array names one. Nothing has to cross between parts.
All inputs are finite; a program needn't handle non-finite values.
Results may differ from the reference program's by a relative error of at most 0.001.
Values may be sent and summed in bfloat16 or wider, within the bound.
A program may use at most 128 MiB of HBM per device.

```python
import jax
import jax.numpy as jnp

D_MODEL = 2560
Q_DIM = 4096
KV_DIM = 1024
RANK = 64


def levels(stream_key, shape, split, low, top_value):
    factor_of = 1.0
    for dim, parts in split:
        steps = jax.random.uniform(jax.random.fold_in(jax.random.fold_in(stream_key, 6), dim), (parts,), jnp.float32, low / len(split), top_value / len(split))
        factor_of = factor_of * jnp.repeat(jnp.exp(steps), shape[dim] // parts).reshape((-1,) + (1,) * (len(shape) - 1 - dim))
    return factor_of


def normal_values(key, dims, scale, reach, split=(), dtype=jnp.bfloat16):
    level = levels(key, dims, split, -0.22, 0.18) if split else 1.0
    entries = jax.random.normal(key, dims, jnp.float32) * scale * level
    return jnp.minimum(jnp.maximum(entries, -reach), reach).astype(dtype)


def setup_inputs(seed: int = 0, part: int = 0) -> dict:
    keys = jax.random.split(jax.random.key(seed), 12)
    own_keys = jax.random.split(jax.random.fold_in(keys[11], part), 12)
    weight_query = normal_values(own_keys[0], (D_MODEL, Q_DIM), D_MODEL ** -0.5, 0.125, ((0, 4), (1, 2)))
    low_query = normal_values(own_keys[1], (D_MODEL, RANK), D_MODEL ** -0.5, 0.125, ((0, 4),))
    high_query = normal_values(own_keys[2], (RANK, Q_DIM), RANK ** -0.5, 0.75, ((1, 2),))
    weight_key = normal_values(own_keys[3], (D_MODEL, KV_DIM), D_MODEL ** -0.5, 0.125, ((0, 4), (1, 2)))
    low_key = normal_values(own_keys[4], (D_MODEL, RANK), D_MODEL ** -0.5, 0.125, ((0, 4),))
    high_key = normal_values(own_keys[5], (RANK, KV_DIM), RANK ** -0.5, 0.75, ((1, 2),))
    weight_value = normal_values(own_keys[6], (D_MODEL, KV_DIM), D_MODEL ** -0.5, 0.125, ((0, 4), (1, 2)))
    low_value = normal_values(own_keys[7], (D_MODEL, RANK), D_MODEL ** -0.5, 0.125, ((0, 4),))
    high_value = normal_values(own_keys[8], (RANK, KV_DIM), RANK ** -0.5, 0.75, ((1, 2),))
    norm_train = jnp.clip(1.0 + 0.15 * jax.random.normal(own_keys[9], (D_MODEL,), jnp.float32), 0.25, 1.75)
    norm_step = jnp.clip(jax.random.uniform(own_keys[10], (D_MODEL,), jnp.float32, -0.3, 0.3) * levels(own_keys[10], (D_MODEL,), ((0, 8),), -0.4, 0.0), -0.3, 0.3)
    return dict(weight_query=weight_query, low_query=low_query, high_query=high_query, weight_key=weight_key, low_key=low_key, high_key=high_key, weight_value=weight_value, low_value=low_value, high_value=high_value, norm_train=norm_train, norm_step=norm_step)


mix_rate = 1.0


def reference(weight_query, low_query, high_query, weight_key, low_key, high_key, weight_value, low_value, high_value, norm_train, norm_step):
    fresh_query = weight_query.astype(jnp.float32) + mix_rate * jnp.dot(low_query, high_query, preferred_element_type=jnp.float32)
    fresh_key = weight_key.astype(jnp.float32) + mix_rate * jnp.dot(low_key, high_key, preferred_element_type=jnp.float32)
    fresh_value = weight_value.astype(jnp.float32) + mix_rate * jnp.dot(low_value, high_value, preferred_element_type=jnp.float32)
    serve_query = fresh_query.T.astype(jnp.bfloat16)
    serve_key = fresh_key.T.astype(jnp.bfloat16)
    serve_value = fresh_value.T.astype(jnp.bfloat16)
    serve_norm = (norm_train + norm_step).astype(jnp.bfloat16)
    return serve_query, serve_key, serve_value, serve_norm
```

```python
import functools

import jax
import jax.numpy as jnp
from jax import lax
from jax.experimental import pallas as pl
from jax.experimental.pallas import tpu as pltpu
from jax.sharding import PartitionSpec as P

mix_rate = 1.0
MESH = pl.DeviceIdType.MESH
IN_VMEM = True


def chunk_rows(widths):
    for rows in (256, 128):
        if all(width % rows == 0 for width in widths):
            return rows
    return None


def gather_kernel(n, tp, rows, *refs):
    weights, low_refs, high_refs = refs[0:3], refs[3:6], refs[6:9]
    norm_ref = refs[9]
    outs = refs[10:13]
    norm_out = refs[13]
    staged, lows, highs = refs[14], refs[15:18], refs[18:21]
    norm_all, load_sem, small_sem, send_sem, recv_sem, norm_send, norm_recv = refs[21:]
    me, my_tp = lax.axis_index("shard"), lax.axis_index("tp")
    right = lax.rem(me + 1, n)
    depth = staged.shape[1]
    counts = [weight.shape[1] // rows for weight in weights]
    starts = [sum(counts[:i]) for i in range(len(counts))]
    total = sum(counts)

    def load(which, c):
        return pltpu.make_async_copy(
            weights[which].at[:, pl.ds(pl.multiple_of(c * rows, rows), rows)],
            staged.at[starts[which] + c],
            load_sem.at[starts[which] + c],
        )

    small = [
        (
            pltpu.make_async_copy(low_refs[i], lows[i], small_sem.at[2 * i]),
            pltpu.make_async_copy(high_refs[i], highs[i], small_sem.at[2 * i + 1]),
        )
        for i in range(3)
    ]
    for which in range(3):
        for copy in small[which]:
            copy.start()

        @pl.loop(0, counts[which])
        def _(c):
            load(which, c).start()

    partners = [(k, t) for k in range(n) for t in range(tp) if (k, t) != (0, 0)]

    def partner(k, t):
        return {"shard": lax.rem(me + k, n), "tp": lax.rem(my_tp + t, tp)}

    barrier = pltpu.get_barrier_semaphore()
    for k, t in partners:
        pl.semaphore_signal(barrier, inc=1, device_id=partner(k, t), device_id_type=MESH)
    pl.semaphore_wait(barrier, len(partners))

    def block(which, c, owner):
        return outs[which].at[
            pl.ds(pl.multiple_of(c * rows, rows), rows),
            pl.ds(pl.multiple_of(owner * depth, 128), depth),
        ]

    def send(which, c, step):
        here = block(which, c, lax.rem(me - step + n, n))
        slot = step * total + starts[which] + c
        return pltpu.make_async_remote_copy(
            here, here, send_sem.at[slot], recv_sem.at[slot],
            device_id={"shard": right}, device_id_type=MESH,
        )

    def arrival(which, c, step):
        here = block(which, c, lax.rem(me - step - 1 + n, n))
        slot = step * total + starts[which] + c
        return pltpu.make_async_remote_copy(
            here, here, send_sem.at[slot], recv_sem.at[slot],
            device_id={"shard": right}, device_id_type=MESH,
        )

    for which in range(3):
        for copy in small[which]:
            copy.wait()

        @pl.loop(0, counts[which])
        def _(c):
            load(which, c).wait()
            high = highs[which][:, pl.ds(pl.multiple_of(c * rows, rows), rows)]
            fresh = staged[starts[which] + c].astype(jnp.float32) + mix_rate * lax.dot_general(
                lows[which][...], high, (((0,), (0,)), ((), ())),
                preferred_element_type=jnp.float32,
            )
            outs[which][
                pl.ds(pl.multiple_of(c * rows, rows), rows),
                pl.ds(pl.multiple_of(me * depth, 128), depth),
            ] = fresh.astype(jnp.bfloat16).T
            send(which, c, 0).start()

    def norm_copy(i, k, t):
        mine = me * tp + my_tp
        return pltpu.make_async_remote_copy(
            norm_ref, norm_all.at[mine], norm_send.at[i], norm_recv.at[i],
            device_id=partner(k, t), device_id_type=MESH,
        )

    def norm_arrival(i, k, t):
        theirs = lax.rem(me - k + n, n) * tp + lax.rem(my_tp - t + tp, tp)
        return pltpu.make_async_remote_copy(
            norm_ref, norm_all.at[theirs], norm_send.at[i], norm_recv.at[i],
            device_id=partner(k, t), device_id_type=MESH,
        )

    for i, (k, t) in enumerate(partners):
        norm_copy(i, k, t).start()
    norm_all[me * tp + my_tp] = norm_ref[...]

    for step in range(n - 1):
        for which in range(3):

            @pl.loop(0, counts[which])
            def _(c):
                arrival(which, c, step).wait_recv()
                if step < n - 2:
                    send(which, c, step + 1).start()

        if step == 0:
            for i, (k, t) in enumerate(partners):
                norm_arrival(i, k, t).wait_recv()
            norm_out[...] = norm_all[...].astype(jnp.bfloat16)

    for step in range(n - 1):
        for which in range(3):

            @pl.loop(0, counts[which])
            def _(c):
                send(which, c, step).wait_send()

    for i, (k, t) in enumerate(partners):
        norm_copy(i, k, t).wait_send()


def gathered(n, tp, rows, weights, lows, highs, norm):
    depth = weights[0].shape[0]
    total = sum(weight.shape[1] // rows for weight in weights)
    group, part = n * tp, norm.shape[1]
    make = pltpu.VMEM if IN_VMEM else jax.ShapeDtypeStruct
    space = pl.BlockSpec(memory_space=pltpu.VMEM if IN_VMEM else pl.ANY)
    vmem, hbm = pl.BlockSpec(memory_space=pltpu.VMEM), pl.BlockSpec(memory_space=pltpu.HBM)
    return pl.pallas_call(
        functools.partial(gather_kernel, n, tp, rows),
        out_shape=[make((weight.shape[1], n * depth), jnp.bfloat16) for weight in weights]
        + [jax.ShapeDtypeStruct((group, 1, part), jnp.bfloat16)],
        in_specs=[hbm] * 9 + [vmem],
        out_specs=[space] * 3 + [vmem],
        scratch_shapes=[
            pltpu.VMEM((total, depth, rows), jnp.bfloat16),
            *[pltpu.VMEM(x.shape, x.dtype) for x in (*lows, *highs)],
            pltpu.VMEM((group, 1, part), jnp.float32),
            pltpu.SemaphoreType.DMA((total,)),
            pltpu.SemaphoreType.DMA((6,)),
            pltpu.SemaphoreType.DMA(((n - 1) * total,)),
            pltpu.SemaphoreType.DMA(((n - 1) * total,)),
            pltpu.SemaphoreType.DMA((group - 1,)),
            pltpu.SemaphoreType.DMA((group - 1,)),
        ],
        compiler_params=pltpu.CompilerParams(
            collective_id=0, has_side_effects=True, vmem_limit_bytes=47 * 2**20
        ),
    )(*weights, *lows, *highs, norm)


def flush_kernel(count, *refs):
    sources, results, sems = refs[:count], refs[count : 2 * count], refs[-1]
    copies = [
        pltpu.make_async_copy(source, result, sems.at[i])
        for i, (source, result) in enumerate(zip(sources, results))
    ]
    for copy in copies:
        copy.start()
    for copy in copies:
        copy.wait()


def flushed(held):
    return pl.pallas_call(
        functools.partial(flush_kernel, len(held)),
        out_shape=[jax.ShapeDtypeStruct(x.shape, x.dtype) for x in held],
        in_specs=[pl.BlockSpec(memory_space=pltpu.VMEM)] * len(held),
        out_specs=[pl.BlockSpec(memory_space=pltpu.HBM)] * len(held),
        scratch_shapes=[pltpu.SemaphoreType.DMA((len(held),))],
        compiler_params=pltpu.CompilerParams(vmem_limit_bytes=2**20),
    )(*held)


def plain(weights, lows, highs, norm_new):
    serve = []
    for weight, low, high in zip(weights, lows, highs):
        fresh = weight.astype(jnp.float32) + mix_rate * jnp.dot(
            low, high, preferred_element_type=jnp.float32
        )
        serve.append(
            lax.all_gather(fresh.astype(jnp.bfloat16), "shard", axis=0, tiled=True).T
        )
    norm = lax.all_gather(
        norm_new.astype(jnp.bfloat16), ("shard", "tp"), axis=0, tiled=True
    )
    return (*serve, norm)


def on_device(n, tp, wq, lq, hq, wk, lk, hk, wv, lv, hv, norm_train, norm_step):
    weights, lows, highs = (wq, wk, wv), (lq, lk, lv), (hq, hk, hv)
    rows = chunk_rows([weight.shape[1] for weight in weights])
    norm_new = norm_train + norm_step
    if n < 2 or rows is None or wq.shape[0] % 128:
        return plain(weights, lows, highs, norm_new)
    *serve, norm = gathered(
        n, tp, rows, weights, [low.T for low in lows], highs, norm_new.reshape(1, -1)
    )
    return (*flushed(serve), norm.reshape(-1))


def solution(mesh):
    in_specs = (
        (P(("trial", "shard"), "tp"), P(("trial", "shard"), None), P("trial", "tp")) * 3
        + (P(("trial", "shard", "tp")),) * 2
    )
    out_specs = (P(("trial", "tp"), None),) * 3 + (P("trial"),)
    body = functools.partial(on_device, mesh.shape["shard"], mesh.shape["tp"])
    return jax.shard_map(
        body, mesh=mesh, in_specs=in_specs, out_specs=out_specs, check_vma=False
    )
```

```python
import functools

import jax
import jax.numpy as jnp
from jax import lax
from jax.experimental import pallas as pl
from jax.experimental.pallas import tpu as pltpu
from jax.sharding import PartitionSpec as P

mix_rate = 1.0
MESH = pl.DeviceIdType.MESH
IN_VMEM = True


def chunk_rows(widths):
    for rows in (256, 128):
        if all(width % rows == 0 for width in widths):
            return rows
    return None


def gather_kernel(n, tp, rows, *refs):
    weights, low_refs, high_refs = refs[0:3], refs[3:6], refs[6:9]
    norm_ref = refs[9]
    outs = refs[10:13]
    norm_out = refs[13]
    staged, lows, highs = refs[14], refs[15:18], refs[18:21]
    norm_all, load_sem, small_sem, send_sem, recv_sem, norm_send, norm_recv = refs[21:]
    me, my_tp = lax.axis_index("shard"), lax.axis_index("tp")
    depth = staged.shape[1]
    counts = [weight.shape[1] // rows for weight in weights]
    starts = [sum(counts[:i]) for i in range(len(counts))]
    total = sum(counts)

    def load(which, c):
        return pltpu.make_async_copy(
            weights[which].at[:, pl.ds(pl.multiple_of(c * rows, rows), rows)],
            staged.at[starts[which] + c],
            load_sem.at[starts[which] + c],
        )

    small = [
        (
            pltpu.make_async_copy(low_refs[i], lows[i], small_sem.at[2 * i]),
            pltpu.make_async_copy(high_refs[i], highs[i], small_sem.at[2 * i + 1]),
        )
        for i in range(3)
    ]
    for which in range(3):
        for copy in small[which]:
            copy.start()

        @pl.loop(0, counts[which])
        def _(c):
            load(which, c).start()

    partners = [(k, t) for k in range(n) for t in range(tp) if (k, t) != (0, 0)]

    def partner(k, t):
        return {"shard": lax.rem(me + k, n), "tp": lax.rem(my_tp + t, tp)}

    barrier = pltpu.get_barrier_semaphore()
    for k, t in partners:
        pl.semaphore_signal(barrier, inc=1, device_id=partner(k, t), device_id_type=MESH)
    pl.semaphore_wait(barrier, len(partners))

    def block(which, c, owner):
        return outs[which].at[
            pl.ds(pl.multiple_of(c * rows, rows), rows),
            pl.ds(pl.multiple_of(owner * depth, 128), depth),
        ]

    def hop(which, c, step, way, owner):
        here = block(which, c, owner)
        slot = ((0 if way > 0 else 1) * (n - 1) + step) * total + starts[which] + c
        return pltpu.make_async_remote_copy(
            here, here, send_sem.at[slot], recv_sem.at[slot],
            device_id={"shard": jnp.clip(me + way, 0, n - 1)}, device_id_type=MESH,
        )

    def sends(step, way):
        owner = me - way * step
        ok = (owner >= 0) & (owner < n) & (me + way >= 0) & (me + way < n)
        return ok, jnp.clip(owner, 0, n - 1)

    def arrives(step, way):
        owner = me - way * (step + 1)
        return (owner >= 0) & (owner < n), jnp.clip(owner, 0, n - 1)

    def send(which, c, step):
        for way in (1, -1):
            ok, owner = sends(step, way)
            pl.when(ok)(lambda: hop(which, c, step, way, owner).start())

    for which in range(3):
        for copy in small[which]:
            copy.wait()

        @pl.loop(0, counts[which])
        def _(c):
            load(which, c).wait()
            high = highs[which][:, pl.ds(pl.multiple_of(c * rows, rows), rows)]
            fresh = staged[starts[which] + c].astype(jnp.float32) + mix_rate * lax.dot_general(
                lows[which][...], high, (((0,), (0,)), ((), ())),
                preferred_element_type=jnp.float32,
            )
            outs[which][
                pl.ds(pl.multiple_of(c * rows, rows), rows),
                pl.ds(pl.multiple_of(me * depth, 128), depth),
            ] = fresh.astype(jnp.bfloat16).T
            send(which, c, 0)

    def norm_copy(i, k, t):
        mine = me * tp + my_tp
        return pltpu.make_async_remote_copy(
            norm_ref, norm_all.at[mine], norm_send.at[i], norm_recv.at[i],
            device_id=partner(k, t), device_id_type=MESH,
        )

    def norm_arrival(i, k, t):
        theirs = lax.rem(me - k + n, n) * tp + lax.rem(my_tp - t + tp, tp)
        return pltpu.make_async_remote_copy(
            norm_ref, norm_all.at[theirs], norm_send.at[i], norm_recv.at[i],
            device_id=partner(k, t), device_id_type=MESH,
        )

    for i, (k, t) in enumerate(partners):
        norm_copy(i, k, t).start()
    norm_all[me * tp + my_tp] = norm_ref[...]

    def pass_on(which, c, step):
        for way in (1, -1):
            ok, owner = arrives(step, way)
            further = ok & (me + way >= 0) & (me + way < n)
            pl.when(ok)(lambda: hop(which, c, step, way, owner).wait_recv())
            if step < n - 2:
                pl.when(further)(lambda: hop(which, c, step + 1, way, owner).start())

    for step in range(n - 1):
        for which in range(3):
            pl.loop(0, counts[which])(functools.partial(pass_on, which, step=step))

        if step == 0:
            for i, (k, t) in enumerate(partners):
                norm_arrival(i, k, t).wait_recv()
            norm_out[...] = norm_all[...].astype(jnp.bfloat16)

    def sent(which, c, step):
        for way in (1, -1):
            ok, owner = sends(step, way)
            pl.when(ok)(lambda: hop(which, c, step, way, owner).wait_send())

    for step in range(n - 1):
        for which in range(3):
            pl.loop(0, counts[which])(functools.partial(sent, which, step=step))

    for i, (k, t) in enumerate(partners):
        norm_copy(i, k, t).wait_send()


def gathered(n, tp, rows, weights, lows, highs, norm):
    depth = weights[0].shape[0]
    total = sum(weight.shape[1] // rows for weight in weights)
    group, part = n * tp, norm.shape[1]
    make = pltpu.VMEM if IN_VMEM else jax.ShapeDtypeStruct
    space = pl.BlockSpec(memory_space=pltpu.VMEM if IN_VMEM else pl.ANY)
    vmem, hbm = pl.BlockSpec(memory_space=pltpu.VMEM), pl.BlockSpec(memory_space=pltpu.HBM)
    return pl.pallas_call(
        functools.partial(gather_kernel, n, tp, rows),
        out_shape=[make((weight.shape[1], n * depth), jnp.bfloat16) for weight in weights]
        + [jax.ShapeDtypeStruct((group, 1, part), jnp.bfloat16)],
        in_specs=[hbm] * 9 + [vmem],
        out_specs=[space] * 3 + [vmem],
        scratch_shapes=[
            pltpu.VMEM((total, depth, rows), jnp.bfloat16),
            *[pltpu.VMEM(x.shape, x.dtype) for x in (*lows, *highs)],
            pltpu.VMEM((group, 1, part), jnp.float32),
            pltpu.SemaphoreType.DMA((total,)),
            pltpu.SemaphoreType.DMA((6,)),
            pltpu.SemaphoreType.DMA((2 * (n - 1) * total,)),
            pltpu.SemaphoreType.DMA((2 * (n - 1) * total,)),
            pltpu.SemaphoreType.DMA((group - 1,)),
            pltpu.SemaphoreType.DMA((group - 1,)),
        ],
        compiler_params=pltpu.CompilerParams(
            collective_id=0, has_side_effects=True, vmem_limit_bytes=47 * 2**20
        ),
    )(*weights, *lows, *highs, norm)


def flush_kernel(count, *refs):
    sources, results, sems = refs[:count], refs[count : 2 * count], refs[-1]
    copies = [
        pltpu.make_async_copy(source, result, sems.at[i])
        for i, (source, result) in enumerate(zip(sources, results))
    ]
    for copy in copies:
        copy.start()
    for copy in copies:
        copy.wait()


def flushed(held):
    return pl.pallas_call(
        functools.partial(flush_kernel, len(held)),
        out_shape=[jax.ShapeDtypeStruct(x.shape, x.dtype) for x in held],
        in_specs=[pl.BlockSpec(memory_space=pltpu.VMEM)] * len(held),
        out_specs=[pl.BlockSpec(memory_space=pltpu.HBM)] * len(held),
        scratch_shapes=[pltpu.SemaphoreType.DMA((len(held),))],
        compiler_params=pltpu.CompilerParams(vmem_limit_bytes=2**20),
    )(*held)


def plain(weights, lows, highs, norm_new):
    serve = []
    for weight, low, high in zip(weights, lows, highs):
        fresh = weight.astype(jnp.float32) + mix_rate * jnp.dot(
            low, high, preferred_element_type=jnp.float32
        )
        serve.append(
            lax.all_gather(fresh.astype(jnp.bfloat16), "shard", axis=0, tiled=True).T
        )
    norm = lax.all_gather(
        norm_new.astype(jnp.bfloat16), ("shard", "tp"), axis=0, tiled=True
    )
    return (*serve, norm)


def on_device(n, tp, wq, lq, hq, wk, lk, hk, wv, lv, hv, norm_train, norm_step):
    weights, lows, highs = (wq, wk, wv), (lq, lk, lv), (hq, hk, hv)
    rows = chunk_rows([weight.shape[1] for weight in weights])
    norm_new = norm_train + norm_step
    if n < 2 or rows is None or wq.shape[0] % 128:
        return plain(weights, lows, highs, norm_new)
    *serve, norm = gathered(
        n, tp, rows, weights, [low.T for low in lows], highs, norm_new.reshape(1, -1)
    )
    return (*flushed(serve), norm.reshape(-1))


def solution(mesh):
    in_specs = (
        (P(("trial", "shard"), "tp"), P(("trial", "shard"), None), P("trial", "tp")) * 3
        + (P(("trial", "shard", "tp")),) * 2
    )
    out_specs = (P(("trial", "tp"), None),) * 3 + (P("trial"),)
    body = functools.partial(on_device, mesh.shape["shard"], mesh.shape["tp"])
    return jax.shard_map(
        body, mesh=mesh, in_specs=in_specs, out_specs=out_specs, check_vma=False
    )
```

```python
import functools

import jax
import jax.numpy as jnp
from jax import lax
from jax.experimental import pallas as pl
from jax.experimental.pallas import tpu as pltpu
from jax.sharding import PartitionSpec as P

mix_rate = 1.0
MESH = pl.DeviceIdType.MESH
IN_VMEM = True


def chunk_rows(widths):
    for rows in (256, 128):
        if all(width % rows == 0 for width in widths):
            return rows
    return None


def gather_kernel(n, tp, rows, *refs):
    weights, low_refs, high_refs = refs[0:3], refs[3:6], refs[6:9]
    norm_train, norm_step = refs[9:11]
    outs = refs[11:14]
    norm_out = refs[14]
    staged, lows, highs = refs[15], refs[16:19], refs[19:22]
    norm_all, load_sem, small_sem, send_sem, recv_sem, norm_send, norm_recv, norm_ref = refs[22:]
    me, my_tp = lax.axis_index("shard"), lax.axis_index("tp")
    depth = staged.shape[1]
    counts = [weight.shape[1] // rows for weight in weights]
    starts = [sum(counts[:i]) for i in range(len(counts))]
    total = sum(counts)

    def load(which, c):
        return pltpu.make_async_copy(
            weights[which].at[:, pl.ds(pl.multiple_of(c * rows, rows), rows)],
            staged.at[starts[which] + c],
            load_sem.at[starts[which] + c],
        )

    small = [
        (
            pltpu.make_async_copy(low_refs[i], lows[i], small_sem.at[2 * i]),
            pltpu.make_async_copy(high_refs[i], highs[i], small_sem.at[2 * i + 1]),
        )
        for i in range(3)
    ]
    for which in range(3):
        for copy in small[which]:
            copy.start()

        @pl.loop(0, counts[which])
        def _(c):
            load(which, c).start()

    partners = [(k, t) for k in range(n) for t in range(tp) if (k, t) != (0, 0)]

    def partner(k, t):
        return {"shard": lax.rem(me + k, n), "tp": lax.rem(my_tp + t, tp)}

    norm_ref[0, :] = norm_train[...] + norm_step[...]
    barrier = pltpu.get_barrier_semaphore()
    for k, t in partners:
        pl.semaphore_signal(barrier, inc=1, device_id=partner(k, t), device_id_type=MESH)
    pl.semaphore_wait(barrier, len(partners))

    def block(which, c, owner):
        return outs[which].at[
            pl.ds(pl.multiple_of(c * rows, rows), rows),
            pl.ds(pl.multiple_of(owner * depth, 128), depth),
        ]

    def hop(which, c, step, way, owner):
        here = block(which, c, owner)
        slot = ((0 if way > 0 else 1) * (n - 1) + step) * total + starts[which] + c
        return pltpu.make_async_remote_copy(
            here, here, send_sem.at[slot], recv_sem.at[slot],
            device_id={"shard": jnp.clip(me + way, 0, n - 1)}, device_id_type=MESH,
        )

    def sends(step, way):
        owner = me - way * step
        ok = (owner >= 0) & (owner < n) & (me + way >= 0) & (me + way < n)
        return ok, jnp.clip(owner, 0, n - 1)

    def arrives(step, way):
        owner = me - way * (step + 1)
        return (owner >= 0) & (owner < n), jnp.clip(owner, 0, n - 1)

    def send(which, c, step):
        for way in (1, -1):
            ok, owner = sends(step, way)
            pl.when(ok)(lambda: hop(which, c, step, way, owner).start())

    for which in range(3):
        for copy in small[which]:
            copy.wait()

        @pl.loop(0, counts[which])
        def _(c):
            load(which, c).wait()
            high = highs[which][:, pl.ds(pl.multiple_of(c * rows, rows), rows)]
            fresh = staged[starts[which] + c].astype(jnp.float32) + mix_rate * lax.dot_general(
                lows[which][...], high, (((0,), (0,)), ((), ())),
                preferred_element_type=jnp.float32,
            )
            outs[which][
                pl.ds(pl.multiple_of(c * rows, rows), rows),
                pl.ds(pl.multiple_of(me * depth, 128), depth),
            ] = fresh.astype(jnp.bfloat16).T
            send(which, c, 0)

    def norm_copy(i, k, t):
        mine = me * tp + my_tp
        return pltpu.make_async_remote_copy(
            norm_ref, norm_all.at[mine], norm_send.at[i], norm_recv.at[i],
            device_id=partner(k, t), device_id_type=MESH,
        )

    def norm_arrival(i, k, t):
        theirs = lax.rem(me - k + n, n) * tp + lax.rem(my_tp - t + tp, tp)
        return pltpu.make_async_remote_copy(
            norm_ref, norm_all.at[theirs], norm_send.at[i], norm_recv.at[i],
            device_id=partner(k, t), device_id_type=MESH,
        )

    for i, (k, t) in enumerate(partners):
        norm_copy(i, k, t).start()
    norm_all[me * tp + my_tp] = norm_ref[...]

    def pass_on(which, c, step):
        for way in (1, -1):
            ok, owner = arrives(step, way)
            further = ok & (me + way >= 0) & (me + way < n)
            pl.when(ok)(lambda: hop(which, c, step, way, owner).wait_recv())
            if step < n - 2:
                pl.when(further)(lambda: hop(which, c, step + 1, way, owner).start())

    for step in range(n - 1):
        for which in range(3):
            pl.loop(0, counts[which])(functools.partial(pass_on, which, step=step))

        if step == 0:
            for i, (k, t) in enumerate(partners):
                norm_arrival(i, k, t).wait_recv()
            norm_out[...] = norm_all[...].astype(jnp.bfloat16)

    def sent(which, c, step):
        for way in (1, -1):
            ok, owner = sends(step, way)
            pl.when(ok)(lambda: hop(which, c, step, way, owner).wait_send())

    for step in range(n - 1):
        for which in range(3):
            pl.loop(0, counts[which])(functools.partial(sent, which, step=step))

    for i, (k, t) in enumerate(partners):
        norm_copy(i, k, t).wait_send()


def gathered(n, tp, rows, weights, lows, highs, train, step):
    depth = weights[0].shape[0]
    total = sum(weight.shape[1] // rows for weight in weights)
    group, part = n * tp, train.shape[0]
    make = pltpu.VMEM if IN_VMEM else jax.ShapeDtypeStruct
    space = pl.BlockSpec(memory_space=pltpu.VMEM if IN_VMEM else pl.ANY)
    vmem, hbm = pl.BlockSpec(memory_space=pltpu.VMEM), pl.BlockSpec(memory_space=pltpu.HBM)
    return pl.pallas_call(
        functools.partial(gather_kernel, n, tp, rows),
        out_shape=[make((weight.shape[1], n * depth), jnp.bfloat16) for weight in weights]
        + [jax.ShapeDtypeStruct((group, 1, part), jnp.bfloat16)],
        in_specs=[hbm] * 9 + [vmem] * 2,
        out_specs=[space] * 3 + [vmem],
        scratch_shapes=[
            pltpu.VMEM((total, depth, rows), jnp.bfloat16),
            *[pltpu.VMEM(x.shape, x.dtype) for x in (*lows, *highs)],
            pltpu.VMEM((group, 1, part), jnp.float32),
            pltpu.SemaphoreType.DMA((total,)),
            pltpu.SemaphoreType.DMA((6,)),
            pltpu.SemaphoreType.DMA((2 * (n - 1) * total,)),
            pltpu.SemaphoreType.DMA((2 * (n - 1) * total,)),
            pltpu.SemaphoreType.DMA((group - 1,)),
            pltpu.SemaphoreType.DMA((group - 1,)),
            pltpu.VMEM((1, part), jnp.float32),
        ],
        compiler_params=pltpu.CompilerParams(
            collective_id=0, has_side_effects=True, vmem_limit_bytes=47 * 2**20
        ),
    )(*weights, *lows, *highs, train, step)


def flush_kernel(count, *refs):
    sources, results, sems = refs[:count], refs[count : 2 * count], refs[-1]
    copies = [
        pltpu.make_async_copy(source, result, sems.at[i])
        for i, (source, result) in enumerate(zip(sources, results))
    ]
    for copy in copies:
        copy.start()
    for copy in copies:
        copy.wait()


def flushed(held):
    return pl.pallas_call(
        functools.partial(flush_kernel, len(held)),
        out_shape=[jax.ShapeDtypeStruct(x.shape, x.dtype) for x in held],
        in_specs=[pl.BlockSpec(memory_space=pltpu.VMEM)] * len(held),
        out_specs=[pl.BlockSpec(memory_space=pltpu.HBM)] * len(held),
        scratch_shapes=[pltpu.SemaphoreType.DMA((len(held),))],
        compiler_params=pltpu.CompilerParams(vmem_limit_bytes=2**20),
    )(*held)


def plain(weights, lows, highs, norm_new):
    serve = []
    for weight, low, high in zip(weights, lows, highs):
        fresh = weight.astype(jnp.float32) + mix_rate * jnp.dot(
            low, high, preferred_element_type=jnp.float32
        )
        serve.append(
            lax.all_gather(fresh.astype(jnp.bfloat16), "shard", axis=0, tiled=True).T
        )
    norm = lax.all_gather(
        norm_new.astype(jnp.bfloat16), ("shard", "tp"), axis=0, tiled=True
    )
    return (*serve, norm)


def on_device(n, tp, wq, lq, hq, wk, lk, hk, wv, lv, hv, norm_train, norm_step):
    weights, lows, highs = (wq, wk, wv), (lq, lk, lv), (hq, hk, hv)
    rows = chunk_rows([weight.shape[1] for weight in weights])
    if n < 2 or rows is None or wq.shape[0] % 128:
        return plain(weights, lows, highs, norm_train + norm_step)
    *serve, norm = gathered(
        n, tp, rows, weights, [low.T for low in lows], highs, norm_train, norm_step
    )
    return (*flushed(serve), norm.reshape(-1))


def solution(mesh):
    in_specs = (
        (P(("trial", "shard"), "tp"), P(("trial", "shard"), None), P("trial", "tp")) * 3
        + (P(("trial", "shard", "tp")),) * 2
    )
    out_specs = (P(("trial", "tp"), None),) * 3 + (P("trial"),)
    body = functools.partial(on_device, mesh.shape["shard"], mesh.shape["tp"])
    return jax.shard_map(
        body, mesh=mesh, in_specs=in_specs, out_specs=out_specs, check_vma=False
    )
```
